32 devices in a mesh: dp: 4 (over x, y), tp: 8 (over z, core).
Axes of the slice: x: 2, y: 2, z: 4, core: 2. Of those that a mesh axis runs over, the one named last changes fastest.
Arguments:
- x: bfloat16 [8192, 5120], P('dp'), parts along dimension 0
- w_gate: bfloat16 [5120, 32768], P(None, 'tp')
- w_up: bfloat16 [5120, 32768], P(None, 'tp')
- w_down: bfloat16 [32768, 5120], P('tp')
Outputs:
- output: bfloat16 [8192, 5120], P('dp'), parts along dimension 0
There are 4 independent parts. The reference program is written for one: setup_inputs(seed, part) draws one part's arguments, and reference() takes and returns one part's arrays. A program takes and returns all parts, laid end to end along the dimension named above; an argument that names none is the same for every part.
All inputs are finite; a program needn't handle non-finite values.
Results may differ from the reference program's by a relative error of at most 0.016.
Values are sent between devices in bfloat16 or wider.
A program may use at most 2 GiB of HBM per device.

```python
import jax
import jax.numpy as jnp

ROWS = 2048
D = 5120
FF = 32768


def setup_inputs(seed: int = 0, part: int = 0) -> dict:
    kx, kg, ku, kd = jax.random.split(jax.random.key(seed), 4)
    drawn = {
        "x": jax.random.normal(jax.random.fold_in(kx, part), (ROWS, D), jnp.float32),
        "w_gate": jax.random.normal(kg, (D, FF), jnp.float32) * D**-0.5,
        "w_up": jax.random.normal(ku, (D, FF), jnp.float32) * D**-0.5,
        "w_down": jax.random.normal(kd, (FF, D), jnp.float32) * FF**-0.5,
    }
    return {k: v.astype(jnp.bfloat16) for k, v in drawn.items()}


def reference(x, w_gate, w_up, w_down):
    gate = jnp.dot(x, w_gate, preferred_element_type=jnp.float32)
    up = jnp.dot(x, w_up, preferred_element_type=jnp.float32)
    hidden = (jax.nn.silu(gate) * up).astype(jnp.bfloat16)
    return jnp.dot(hidden, w_down, preferred_element_type=jnp.float32).astype(jnp.bfloat16)
```

```python
import jax
import jax.numpy as jnp
from jax import lax
from jax.experimental import pallas as pl
from jax.experimental.pallas import tpu as pltpu
from jax.sharding import PartitionSpec as P

MESH = pl.DeviceIdType.MESH
BF, F32 = jnp.bfloat16, jnp.float32

CH = 512
TG = 256
TD = 512
HALF = 128

L1, L2, L3, L4, L5 = 2, 4, 6, 8, 10
NS = 8
NK = 7
NG = 3
NX = 4


def kernel(x, wg, wu, wd, y, xb, gb, ub, db, hid, keep, xs, xr, es, er, ms, mr, ys,
           xsem, gsem, usem, dsem, xs_s, xr_s, es_s, er_s, ms_s, mr_s, ys_s, yo_s, ye_s, yp_s, fw_s):
    rows, width = x.shape
    ff = wg.shape[1]
    nch, ng, nd = rows // CH, ff // TG, width // TD
    npairs = nch * nd
    t_idx = lax.axis_index("tp")
    z, c = t_idx // 2, t_idx % 2
    side = z // 2
    mid = (z == 1) | (z == 2)
    end = jnp.logical_not(mid)
    partner = {"tp": z * 2 + 1 - c}
    inner = {"tp": (1 + side) * 2 + c}
    outer = {"tp": 3 * side * 2 + c}
    across = {"tp": (2 - side) * 2 + c}

    def remote(src, dst, ssem, rsem, dev):
        return pltpu.make_async_remote_copy(
            src_ref=src, dst_ref=dst, send_sem=ssem, recv_sem=rsem, device_id=dev, device_id_type=MESH
        )

    def sl(q, n):
        return lax.rem(q + 8 * n, n)

    def x_copy(ch):
        b = lax.rem(ch, 2)
        return pltpu.make_async_copy(x.at[pl.ds(ch * CH, CH), :], xb.at[b], xsem.at[b])

    def g_copies(g):
        cols = pl.ds(pl.multiple_of(lax.rem(g, ng) * TG, TG), TG)
        s = lax.rem(g, NG)
        return (
            pltpu.make_async_copy(wg.at[:, cols], gb.at[s], gsem.at[s]),
            pltpu.make_async_copy(wu.at[:, cols], ub.at[s], usem.at[s]),
        )

    def d_copy(d):
        cols = pl.ds(pl.multiple_of(lax.rem(d, nd) * TD, TD), TD)
        s = lax.rem(d, 2)
        return pltpu.make_async_copy(wd.at[:, cols], db.at[s], dsem.at[s])

    def g_top(g):
        for cp in g_copies(g):
            cp.wait()

        @pl.when(g + NG - 1 < nch * ng)
        def _():
            for cp in g_copies(g + NG - 1):
                cp.start()

    def d_top(d):
        d_copy(d).wait()

        @pl.when(d + 1 < npairs)
        def _():
            d_copy(d + 1).start()

    def g_body(g):
        s, par = lax.rem(g, NG), lax.rem(g // ng, 2)
        gate = jnp.dot(xb[par], gb[s], preferred_element_type=F32)
        up = jnp.dot(xb[par], ub[s], preferred_element_type=F32)
        cols = pl.ds(pl.multiple_of(lax.rem(g, ng) * TG, TG), TG)
        hid[par, :, cols] = (gate * jax.nn.sigmoid(gate) * up).astype(BF)

    def d_body(d):
        part = jnp.dot(hid[lax.rem(d // nd, 2)], db[lax.rem(d, 2)], preferred_element_type=F32)
        s, sx = lax.rem(d, NK), lax.rem(d, NX)
        for u in range(2):
            a = part[2 * u * HALF : (2 * u + 1) * HALF]
            b = part[(2 * u + 1) * HALF : (2 * u + 2) * HALF]
            keep[s, u] = jnp.where(c == 0, a, b)
            xs[sx, u] = jnp.where(c == 0, b, a).astype(BF)

    def place(q, piece, n=1):
        row = (q // nd) * CH + piece * 2 * HALF + c * HALF
        return y.at[
            pl.ds(pl.multiple_of(row, HALF), n * HALF),
            pl.ds(pl.multiple_of(lax.rem(q, nd) * TD, TD), TD),
        ]

    def swap(q):
        sx, s = sl(q, NX), sl(q, NS)
        return remote(xs.at[sx], xr.at[s], xs_s.at[sx], xr_s.at[s], partner)

    def inward(q):
        sx, s = sl(q, NX), sl(q, NS)
        return remote(es.at[sx], er.at[s], es_s.at[sx], er_s.at[s], inner)

    def cross(q):
        sx, s = sl(q, NX), sl(q, NS)
        return remote(ms.at[sx], mr.at[s], ms_s.at[sx], mr_s.at[s], across)

    def finals(q):
        sx = sl(q, NX)
        dst = place(q, side)
        return (
            remote(ys.at[sx], dst, ys_s.at[sx, 0], yo_s.at[q], across),
            remote(ys.at[sx], dst, ys_s.at[sx, 1], ye_s.at[q, 0], outer),
            remote(ys.at[sx], dst, ys_s.at[sx, 2], yp_s.at[q, 0], partner),
            pltpu.make_async_copy(ys.at[sx], dst, ys_s.at[sx, 3]),
        )

    def sent_finals(q):
        cps = finals(q)
        for cp in cps[:3]:
            cp.wait_send()
        cps[3].wait()

    def from_across(q):
        ref = place(q, 1 - side)
        return remote(ref, ref, fw_s.at[0], yo_s.at[q], across)

    def mid_forward(q):
        ref = place(q, 1 - side)
        return (
            remote(ref, ref, fw_s.at[0], ye_s.at[q, 1], outer),
            remote(ref, ref, fw_s.at[1], yp_s.at[q, 1], partner),
        )

    def end_forward(q):
        return [
            remote(place(q, p), place(q, p), fw_s.at[k], yp_s.at[q, k], partner)
            for k, p in ((0, side), (1, 1 - side))
        ]

    def end_arrivals(q):
        return [
            remote(place(q, p), place(q, p), fw_s.at[k], ye_s.at[q, k], inner)
            for k, p in ((0, side), (1, 1 - side))
        ]

    def held(q):
        return jnp.where(q < 0, NS, lax.rem(q + NS, NS))

    def live(q):
        return (q >= 0) & (q < npairs)

    def arrive(t):
        @pl.when(live(t - L4) & mid)
        def _():
            from_across(t - L4).wait_recv()
            for cp in mid_forward(t - L4):
                cp.start()

        @pl.when(live(t - L5) & end)
        def _():
            for cp in end_arrivals(t - L5):
                cp.wait_recv()
            for cp in end_forward(t - L5):
                cp.start()

        @pl.when(live(t - NX))
        def _():
            swap(t - NX).wait_send()

        @pl.when(live(t - L1 - NX) & end)
        def _():
            inward(t - L1 - NX).wait_send()

        @pl.when(live(t - L2 - NX) & mid)
        def _():
            cross(t - L2 - NX).wait_send()

        @pl.when(live(t - L3 - NX) & mid)
        def _():
            sent_finals(t - L3 - NX)

        @pl.when(live(t - L1))
        def _():
            swap(t - L1).wait_recv()

        @pl.when(live(t - L2) & mid)
        def _():
            inward(t - L2).wait_recv()

        @pl.when(live(t - L3) & mid)
        def _():
            cross(t - L3).wait_recv()

    def leave(t):
        swap(t).start()

        @pl.when(live(t - L1) & end)
        def _():
            inward(t - L1).start()

        @pl.when(live(t - L2) & mid)
        def _():
            cross(t - L2).start()

        @pl.when(live(t - L3) & mid)
        def _():
            for cp in finals(t - L3):
                cp.start()

    def stage1(q):
        s = sl(q, NS)
        es[sl(q, NX)] = (keep[sl(q, NK)] + xr[s].astype(F32)).astype(BF)

    def stage2(q):
        s = sl(q, NS)
        e, k = held(q), sl(q, NK)
        own = keep[k, side] + xr[s, side].astype(F32) + er[e, side].astype(F32)
        far = keep[k, 1 - side] + xr[s, 1 - side].astype(F32) + er[e, 1 - side].astype(F32)
        keep[k, side] = own
        ms[sl(q, NX)] = far.astype(BF)

    def stage3(q):
        ys[sl(q, NX)] = (keep[sl(q, NK), side] + mr[held(q)].astype(F32)).astype(BF)

    def stages(t):
        stage3(t - L3)
        stage2(t - L2)
        stage1(t - L1)

    x_copy(0).start()
    for k in range(NG - 1):
        for cp in g_copies(k):
            cp.start()
    d_copy(0).start()
    barrier = pltpu.get_barrier_semaphore()
    pl.semaphore_signal(barrier, inc=1, device_id=partner, device_id_type=MESH)

    @pl.when(end)
    def _():
        pl.semaphore_signal(barrier, inc=1, device_id=inner, device_id_type=MESH)

    @pl.when(mid)
    def _():
        pl.semaphore_signal(barrier, inc=1, device_id=outer, device_id_type=MESH)
        pl.semaphore_signal(barrier, inc=1, device_id=across, device_id_type=MESH)

    @pl.when(end)
    def _():
        pl.semaphore_wait(barrier, 2)

    @pl.when(mid)
    def _():
        pl.semaphore_wait(barrier, 3)

    x_copy(0).wait()
    x_copy(1).start()

    def first(i, _):
        g_top(i)
        g_body(i)
        return 0

    lax.fori_loop(0, ng, first, 0)

    gh, dh = ng // 2, nd // 2

    def half_chunk(h, _):
        ch = h // 2 + 1

        @pl.when(h % 2 == 0)
        def _():
            x_copy(ch).wait()

            @pl.when(ch + 1 < nch)
            def _():
                x_copy(ch + 1).start()

        def tick(i, _):
            o = (gh * i + dh - 1) // dh
            g, d = ng + h * gh + o, h * dh + i
            arrive(d)
            g_top(g)
            d_top(d)
            g_body(g)
            d_body(d)
            stages(d)
            leave(d)

            @pl.when((gh * (i + 1) + dh - 1) // dh - o == 2)
            def _():
                g_top(g + 1)
                g_body(g + 1)

            return 0

        lax.fori_loop(0, dh, tick, 0)
        return 0

    lax.fori_loop(0, 2 * (nch - 1), half_chunk, 0)

    t0 = (nch - 1) * nd

    def upto(i, done, goal, by):
        return jnp.minimum(jnp.minimum(t0 - done + by * i, t0 - goal + i), npairs)

    def ranged(i, done, goal, body):
        lax.fori_loop(upto(i, done, goal, 2), upto(i + 1, done, goal, 2), body, 0)

    def tail(i, _):
        d = t0 + i

        @pl.when(d < npairs)
        def _():
            d_top(d)
            swap(d - NX).wait_send()
            d_body(d)
            swap(d).start()

        def one(q, _):
            swap(q).wait_recv()

            @pl.when(end)
            def _():
                inward(q - NX).wait_send()
                stage1(q)
                inward(q).start()

            return 0

        def two(q, _):
            inward(q).wait_recv()
            cross(q - NX).wait_send()
            stage2(q)
            cross(q).start()
            return 0

        def three(q, _):
            cross(q).wait_recv()
            sent_finals(q - NX)
            stage3(q)
            for cp in finals(q):
                cp.start()
            return 0

        def four(q, _):
            from_across(q).wait_recv()
            for cp in mid_forward(q):
                cp.start()
            return 0

        def five(q, _):
            for cp in end_arrivals(q):
                cp.wait_recv()
            for cp in end_forward(q):
                cp.start()
            return 0

        @pl.when(end)
        def _():
            ranged(i, L5, L2 + 6, five)

        ranged(i, L1, 1, one)

        @pl.when(mid)
        def _():
            ranged(i, L2, L2, two)
            ranged(i, L3, L2 + 1, three)
            ranged(i, L4, L2 + 3, four)

        return 0

    lax.fori_loop(0, nd + L2 + 6, tail, 0)

    for q in range(npairs - NX, npairs):
        swap(q).wait_send()

        @pl.when(end)
        def _():
            inward(q).wait_send()

        @pl.when(mid)
        def _():
            cross(q).wait_send()
            sent_finals(q)

    def arrivals(q, _):
        for k in range(2):
            remote(place(q, 0), place(q, 0), fw_s.at[0], yp_s.at[q, k], partner).wait_recv()
        return 0

    lax.fori_loop(0, npairs, arrivals, 0)
    for k in range(2):
        ref = y.at[pl.ds(0, npairs * HALF * TD // width), :]
        remote(ref, ref, fw_s.at[k], yp_s.at[0, 0], partner).wait_send()


def block(x, w_gate, w_up, w_down):
    rows, width = x.shape
    ff = w_gate.shape[1]
    npairs = (rows // CH) * (width // TD)
    vm = pltpu.VMEM
    dma = pltpu.SemaphoreType.DMA
    return pl.pallas_call(
        kernel,
        out_shape=jax.ShapeDtypeStruct((rows, width), BF),
        in_specs=[pl.BlockSpec(memory_space=pl.ANY)] * 4,
        out_specs=pl.BlockSpec(memory_space=pl.ANY),
        scratch_shapes=[
            vm((2, CH, width), BF),
            vm((NG, width, TG), BF),
            vm((NG, width, TG), BF),
            vm((2, ff, TD), BF),
            vm((2, CH, ff), BF),
            vm((NK, 2, HALF, TD), F32),
            vm((NX, 2, HALF, TD), BF),
            vm((NS, 2, HALF, TD), BF),
            vm((NX, 2, HALF, TD), BF),
            vm((NS + 1, 2, HALF, TD), BF),
            vm((NX, HALF, TD), BF),
            vm((NS + 1, HALF, TD), BF),
            vm((NX, HALF, TD), BF),
            dma((2,)),
            dma((NG,)),
            dma((NG,)),
            dma((2,)),
            dma((NX,)),
            dma((NS,)),
            dma((NX,)),
            dma((NS,)),
            dma((NX,)),
            dma((NS,)),
            dma((NX, 4)),
            dma((npairs,)),
            dma((npairs, 2)),
            dma((npairs, 2)),
            dma((2,)),
        ],
        compiler_params=pltpu.CompilerParams(
            collective_id=0, has_side_effects=True, vmem_limit_bytes=67043328
        ),
    )(x, w_gate, w_up, w_down)


def solution(mesh):
    return jax.shard_map(
        block,
        mesh=mesh,
        in_specs=(P("dp", None), P(None, "tp"), P(None, "tp"), P("tp", None)),
        out_specs=P("dp", None),
        check_vma=False,
    )
```
